128 devices in a mesh: dp: 1, cp: 128 (over z, y, x, core).
Axes of the slice: x: 4, y: 4, z: 4, core: 2. Of those that a mesh axis runs over, the one named last changes fastest.
Arguments:
- hidden: bfloat16 [16384, 4096], P(('dp', 'cp'))
- grad_out: bfloat16 [16384, 4096], P(('dp', 'cp'))
- w_query: bfloat16 [4096, 8, 128], replicated
- w_key: bfloat16 [4096, 2, 128], replicated
- w_value: bfloat16 [4096, 2, 128], replicated
- w_out: bfloat16 [8, 128, 4096], replicated
Outputs:
- output 1: bfloat16 [16384, 4096], P(('dp', 'cp'))
- output 2: bfloat16 [16384, 4096], P(('dp', 'cp'))
- output 3: float32 [4096, 8, 128], P('dp')
- output 4: float32 [4096, 2, 128], P('dp')
- output 5: float32 [4096, 2, 128], P('dp')
- output 6: float32 [8, 128, 4096], P('dp')
All inputs are finite; a program needn't handle non-finite values.
Results may differ from the reference program's by a relative error of at most 0.010151.
Values are sent between devices in bfloat16 or wider.
A program may use at most 1 GiB of HBM per device.

```python
import jax
import jax.numpy as jnp
from jax import lax

TOKENS_DEV = 128
CP = 128
D = 4096
HEADS = 8
KV_HEADS = 2
HEAD = 128


def setup_inputs(seed: int = 0, part: int = 0) -> dict:
    seq_len = TOKENS_DEV * CP
    part_key = jax.random.fold_in(jax.random.key(seed), part)
    key_hidden, key_grad = jax.random.split(part_key)
    key_wq, key_wk, key_wv, key_wo = jax.random.split(jax.random.key(seed + 1), 4)
    hidden = jax.random.normal(key_hidden, (seq_len, D), jnp.float32)
    grad_out = jax.random.normal(key_grad, (seq_len, D), jnp.float32)
    w_query = jax.random.normal(key_wq, (D, HEADS, HEAD), jnp.float32) * D ** -0.5
    w_key = jax.random.normal(key_wk, (D, KV_HEADS, HEAD), jnp.float32) * D ** -0.5
    w_value = jax.random.normal(key_wv, (D, KV_HEADS, HEAD), jnp.float32) * D ** -0.5
    w_out = jax.random.normal(key_wo, (HEADS, HEAD, D), jnp.float32) * (HEADS * HEAD) ** -0.5
    return {
        "hidden": hidden.astype(jnp.bfloat16),
        "grad_out": grad_out.astype(jnp.bfloat16),
        "w_query": w_query.astype(jnp.bfloat16),
        "w_key": w_key.astype(jnp.bfloat16),
        "w_value": w_value.astype(jnp.bfloat16),
        "w_out": w_out.astype(jnp.bfloat16),
    }


def token_positions():
    half_len = TOKENS_DEV // 2
    row_ids = jnp.arange(TOKENS_DEV * CP)
    owner_dev = row_ids // TOKENS_DEV
    within = row_ids % TOKENS_DEV
    block_idx = jnp.where(within < half_len, owner_dev, 2 * CP - 1 - owner_dev)
    return block_idx * half_len + within % half_len


def reference(hidden, grad_out, w_query, w_key, w_value, w_out):
    seq_len = TOKENS_DEV * CP
    half_len = TOKENS_DEV // 2
    num_blocks = 2 * CP
    group_size = HEADS // KV_HEADS
    score_scale = HEAD ** -0.5
    positions = token_positions()
    wq_flat = w_query.reshape(D, HEADS * HEAD)
    wk_flat = w_key.reshape(D, KV_HEADS * HEAD)
    wv_flat = w_value.reshape(D, KV_HEADS * HEAD)
    wo_flat = w_out.reshape(HEADS * HEAD, D)
    query_all = jnp.dot(hidden, wq_flat, preferred_element_type=jnp.float32).astype(jnp.bfloat16)
    keys_all = jnp.dot(hidden, wk_flat, preferred_element_type=jnp.float32).astype(jnp.bfloat16)
    values_all = jnp.dot(hidden, wv_flat, preferred_element_type=jnp.float32).astype(jnp.bfloat16)
    keys_wide = keys_all.reshape(seq_len, KV_HEADS, HEAD).astype(jnp.float32)
    values_wide = values_all.reshape(seq_len, KV_HEADS, HEAD).astype(jnp.float32)
    query_blocks = query_all.reshape(num_blocks, half_len, KV_HEADS, group_size, HEAD)
    pos_blocks = positions.reshape(num_blocks, half_len)

    def masked_scores(query_block, pos_block):
        scores = jnp.einsum("qkgd,skd->kgqs", query_block.astype(jnp.float32), keys_wide) * score_scale
        visible = pos_block[:, None] >= positions[None, :]
        return jnp.where(visible, scores, -jnp.inf)

    def forward_block(items):
        query_block, pos_block = items
        masked = masked_scores(query_block, pos_block)
        log_norm = jax.nn.logsumexp(masked, axis=-1)
        att_probs = jnp.exp(masked - log_norm[..., None]).astype(jnp.bfloat16)
        attended = jnp.einsum("kgqs,skd->qkgd", att_probs.astype(jnp.float32), values_wide)
        return attended.astype(jnp.bfloat16), log_norm

    att_blocks, norm_blocks = lax.map(forward_block, (query_blocks, pos_blocks))
    attended = att_blocks.reshape(seq_len, HEADS * HEAD)
    output = jnp.dot(attended, wo_flat, preferred_element_type=jnp.float32).astype(jnp.bfloat16)
    d_att = jnp.dot(grad_out, wo_flat.T, preferred_element_type=jnp.float32).astype(jnp.bfloat16)
    delta_rows = jnp.sum(
        d_att.astype(jnp.float32).reshape(seq_len, KV_HEADS, group_size, HEAD)
        * attended.astype(jnp.float32).reshape(seq_len, KV_HEADS, group_size, HEAD),
        axis=-1,
    )
    delta_blocks = jnp.transpose(delta_rows.reshape(num_blocks, half_len, KV_HEADS, group_size), (0, 2, 3, 1))
    dout_blocks = d_att.reshape(num_blocks, half_len, KV_HEADS, group_size, HEAD)

    def backward_block(carry, items):
        key_acc, value_acc = carry
        query_block, pos_block, log_norm, dout_block, delta_block = items
        masked = masked_scores(query_block, pos_block)
        att_probs = jnp.exp(masked - log_norm[..., None]).astype(jnp.bfloat16).astype(jnp.float32)
        dout_wide = dout_block.astype(jnp.float32)
        d_probs = jnp.einsum("qkgd,skd->kgqs", dout_wide, values_wide)
        d_scores = (att_probs * (d_probs - delta_block[..., None])).astype(jnp.bfloat16).astype(jnp.float32)
        query_grad = (jnp.einsum("kgqs,skd->qkgd", d_scores, keys_wide) * score_scale).astype(jnp.bfloat16)
        key_acc = key_acc + jnp.einsum("kgqs,qkgd->skd", d_scores, query_block.astype(jnp.float32)) * score_scale
        value_acc = value_acc + jnp.einsum("kgqs,qkgd->skd", att_probs, dout_wide)
        return (key_acc, value_acc), query_grad

    zero_acc = jnp.zeros((seq_len, KV_HEADS, HEAD), jnp.float32)
    (key_sum, value_sum), query_grads = lax.scan(
        backward_block, (zero_acc, zero_acc), (query_blocks, pos_blocks, norm_blocks, dout_blocks, delta_blocks)
    )
    query_grad = query_grads.reshape(seq_len, HEADS * HEAD)
    key_grad = key_sum.astype(jnp.bfloat16).reshape(seq_len, KV_HEADS * HEAD)
    value_grad = value_sum.astype(jnp.bfloat16).reshape(seq_len, KV_HEADS * HEAD)
    grad_hidden = (
        jnp.dot(query_grad, wq_flat.T, preferred_element_type=jnp.float32)
        + jnp.dot(key_grad, wk_flat.T, preferred_element_type=jnp.float32)
        + jnp.dot(value_grad, wv_flat.T, preferred_element_type=jnp.float32)
    ).astype(jnp.bfloat16)
    grad_w_query = jnp.dot(hidden.T, query_grad, preferred_element_type=jnp.float32).reshape(D, HEADS, HEAD)
    grad_w_key = jnp.dot(hidden.T, key_grad, preferred_element_type=jnp.float32).reshape(D, KV_HEADS, HEAD)
    grad_w_value = jnp.dot(hidden.T, value_grad, preferred_element_type=jnp.float32).reshape(D, KV_HEADS, HEAD)
    grad_w_out = jnp.dot(attended.T, grad_out, preferred_element_type=jnp.float32).reshape(HEADS, HEAD, D)
    return (output, grad_hidden, grad_w_query, grad_w_key, grad_w_value, grad_w_out)
```

```python
import functools
import math

import jax
import jax.numpy as jnp
from jax import lax
from jax.experimental import pallas as pl
from jax.experimental.layout import Layout, with_layout_constraint
from jax.experimental.pallas import tpu as pltpu
from jax.sharding import PartitionSpec as P

F32, BF16 = jnp.float32, jnp.bfloat16
DEVS_PER_TILE = 8
PLANES = 4
NT = (((1,), (1,)), ((), ()))
TN = (((0,), (0,)), ((), ()))
NN = (((1,), (0,)), ((), ()))


def dot(a, b, dims):
    return lax.dot_general(a, b, dims, preferred_element_type=F32)


def stack_heads(ref, half_len, group, head_dim):
    parts = []
    for half in (1, 0):
        for g in range(group):
            parts.append(ref[half * half_len:(half + 1) * half_len, g * head_dim:(g + 1) * head_dim])
    return jnp.concatenate(parts, axis=0)


def unstack_heads(ref, rows, half_len, group, head_dim):
    for i, half in enumerate((1, 0)):
        for g in range(group):
            block = rows[(i * group + g) * half_len:(i * group + g + 1) * half_len]
            ref[half * half_len:(half + 1) * half_len, g * head_dim:(g + 1) * head_dim] = block


def place(tile, per, plane, layer):
    return pl.ds(tile * per % plane, per), jnp.bitwise_xor(tile * per // plane, layer)


def tile_mask(tile, half, rank, half_len, keys, cols):
    key_dev = tile * (keys // half_len) + lax.broadcasted_iota(jnp.int32, (keys, cols), 0) // half_len
    key_off = lax.broadcasted_iota(jnp.int32, (keys, cols), 0) % half_len
    q_off = lax.broadcasted_iota(jnp.int32, (keys, cols), 1) % half_len
    sign = 1 if half == 0 else -1
    return sign * (rank - key_dev) * half_len + q_off - key_off >= 0


def ranks_of(devs, plane):
    me = lax.axis_index("cp")
    layer = me // plane
    mirror = (PLANES - 1 - layer) * plane + me % plane
    return layer, jnp.where(pl.program_id(0) == 0, me, mirror)


def fwd_kernel(devs, half_len, group, head_dim, scale2, q_ref, kv_ref, do_ref, o_ref, stats_ref, qs, m_ref, l_ref, acc):
    plane = devs // PLANES
    layer, rank = ranks_of(devs, plane)
    per = min(DEVS_PER_TILE, plane)
    tiles = devs // per
    diag = rank // per
    nq = group * half_len
    keys = per * half_len
    k_cols, v_cols = pl.ds(0, head_dim), pl.ds(head_dim, head_dim)
    qs[...] = stack_heads(q_ref, half_len, group, head_dim)

    def update(k, v, cols, mask, first=False):
        s = dot(k, qs[cols, :], NT) * scale2
        if mask is not None:
            s = jnp.where(mask, s, -jnp.inf)
        top = jnp.max(s, axis=0, keepdims=True)
        if not first:
            old = m_ref[:, cols]
            top = jnp.maximum(old, top)
            shrink = jnp.exp2(old - top)
        p = jnp.exp2(s - top)
        total = jnp.sum(p, axis=0, keepdims=True)
        out = dot(v, p.astype(BF16), TN)
        if not first:
            total = total + l_ref[:, cols] * shrink
            out = out + acc[:, cols] * shrink
        m_ref[:, cols] = top
        l_ref[:, cols] = total
        acc[:, cols] = out

    high, low, every = pl.ds(0, nq), pl.ds(nq, nq), pl.ds(0, 2 * nq)

    def part(kind, tile, half):
        return kv_ref[(*place(tile, per, plane, layer), half, slice(None), kind)].reshape(keys, head_dim)

    def both(kind, tile):
        return kv_ref[(*place(tile, per, plane, layer), slice(None), slice(None), kind)].reshape(2 * keys, head_dim)

    update(part(k_cols, diag, 0), part(v_cols, diag, 0), low, tile_mask(diag, 0, rank, half_len, keys, nq), first=True)
    update(part(k_cols, diag, 0), part(v_cols, diag, 0), high, None, first=True)
    update(part(k_cols, diag, 1), part(v_cols, diag, 1), high, tile_mask(diag, 1, rank, half_len, keys, nq))

    @pl.loop(0, diag)
    def _(t):
        update(part(k_cols, t, 0), part(v_cols, t, 0), every, None)

    @pl.loop(diag + 1, tiles)
    def _(t):
        update(both(k_cols, t), both(v_cols, t), high, None)

    out_t = acc[...] / l_ref[...]
    out = jnp.transpose(out_t).astype(BF16)
    unstack_heads(o_ref, out, half_len, group, head_dim)
    do_t = jnp.transpose(stack_heads(do_ref, half_len, group, head_dim).astype(F32))
    delta = jnp.sum(do_t * out_t.astype(BF16).astype(F32), axis=0, keepdims=True)
    stats_ref[0, 0:1, :] = m_ref[...] + jnp.log2(l_ref[...])
    stats_ref[0, 1:2, :] = delta


def bwd_kernel(devs, half_len, group, head_dim, scale, scale2, q_ref, kv_ref, do_ref, stats_ref,
               dq_ref, dkv_ref, qs, dos, dq_acc):
    plane = devs // PLANES
    layer, rank = ranks_of(devs, plane)
    per = min(DEVS_PER_TILE, plane)
    tiles = devs // per
    diag = rank // per
    nq = group * half_len
    keys = per * half_len
    k_cols, v_cols = pl.ds(0, head_dim), pl.ds(head_dim, head_dim)
    qs[...] = stack_heads(q_ref, half_len, group, head_dim)
    dos[...] = stack_heads(do_ref, half_len, group, head_dim)
    high, every = pl.ds(0, nq), pl.ds(0, 2 * nq)

    def grads(k, v, cols, mask, first=False):
        q, do = qs[cols, :], dos[cols, :]
        s = dot(k, q, NT) * scale2 - stats_ref[0, 0:1, cols]
        if mask is not None:
            s = jnp.where(mask, s, -jnp.inf)
        p = jnp.exp2(s).astype(BF16)
        dv = dot(p, do, NN)
        dp = dot(v, do, NT) - stats_ref[0, 1:2, cols]
        ds = (p.astype(F32) * dp).astype(BF16)
        dk = dot(ds, q, NN) * scale
        dq = dot(k, ds, TN)
        dq_acc[:, cols] = dq if first else dq_acc[:, cols] + dq
        return dk, dv

    def part(kind, tile, half):
        return kv_ref[(*place(tile, per, plane, layer), half, slice(None), kind)].reshape(keys, head_dim)

    def put(tile, half, dk, dv):
        for kind, value in enumerate((dk, dv)):
            where = (*place(tile, per, plane, layer), kind, half)
            dkv_ref[where] = dkv_ref[where] + value.reshape(per, half_len, head_dim)

    @pl.when(pl.program_id(0) == 0)
    def _():
        @pl.loop(0, plane)
        def _(j):
            dkv_ref[j] = jnp.zeros_like(dkv_ref[j])

    mask = jnp.concatenate(
        [jnp.ones((keys, nq), jnp.bool_), tile_mask(diag, 0, rank, half_len, keys, nq)], axis=1)
    dk, dv = grads(part(k_cols, diag, 0), part(v_cols, diag, 0), every, mask, first=True)
    put(diag, 0, dk, dv)
    dk, dv = grads(part(k_cols, diag, 1), part(v_cols, diag, 1), high, tile_mask(diag, 1, rank, half_len, keys, nq))
    put(diag, 1, dk, dv)

    @pl.loop(0, diag)
    def _(t):
        dk, dv = grads(part(k_cols, t, 0), part(v_cols, t, 0), every, None)
        put(t, 0, dk, dv)

    @pl.loop(diag + 1, tiles)
    def _(t):
        where = (*place(t, per, plane, layer), slice(None), slice(None))
        k = kv_ref[(*where, k_cols)].reshape(2 * keys, head_dim)
        v = kv_ref[(*where, v_cols)].reshape(2 * keys, head_dim)
        dk, dv = grads(k, v, high, None)
        dk = dk.reshape(per, 2, half_len, head_dim)
        dv = dv.reshape(per, 2, half_len, head_dim)
        for half in range(2):
            put(t, half, dk[:, half], dv[:, half])

    unstack_heads(dq_ref, jnp.transpose(dq_acc[...] * scale).astype(BF16), half_len, group, head_dim)


def attention_calls(devs, tok, group, head_dim):
    half_len = tok // 2
    plane = devs // PLANES
    scale = head_dim ** -0.5
    scale2 = scale * math.log2(math.e)
    rows = 2 * group * half_len
    wide = group * head_dim
    row_spec = pl.BlockSpec((None, tok, wide), lambda h: (h, 0, 0))
    kv_spec = pl.BlockSpec((plane, PLANES, 2, half_len, 2 * head_dim), lambda h: (0, 0, 0, 0, 0))
    stats_spec = pl.BlockSpec((1, 8, rows), lambda h: (h, 0, 0))
    pairs = 2 * group * half_len * half_len * (2 * devs + 1)
    params = pltpu.CompilerParams(dimension_semantics=("arbitrary",), vmem_limit_bytes=62 * 1024 * 1024)
    kv_bytes = devs * tok * 2 * head_dim * 2
    row_shape = jax.ShapeDtypeStruct((2, tok, wide), BF16)
    forward = pl.pallas_call(
        functools.partial(fwd_kernel, devs, half_len, group, head_dim, scale2),
        grid=(2,),
        in_specs=[row_spec, kv_spec, row_spec],
        out_specs=[row_spec, stats_spec],
        out_shape=[row_shape, jax.ShapeDtypeStruct((2, 8, rows), F32)],
        scratch_shapes=[pltpu.VMEM((rows, head_dim), BF16), pltpu.VMEM((1, rows), F32), pltpu.VMEM((1, rows), F32),
                        pltpu.VMEM((head_dim, rows), F32)],
        compiler_params=params,
        cost_estimate=pl.CostEstimate(flops=pairs * 4 * head_dim, bytes_accessed=kv_bytes, transcendentals=pairs),
        name="attention_forward",
    )
    part_shape = (plane, PLANES, 2, 2, half_len, head_dim)
    backward = pl.pallas_call(
        functools.partial(bwd_kernel, devs, half_len, group, head_dim, scale, scale2),
        grid=(2,),
        in_specs=[row_spec, kv_spec, row_spec, stats_spec],
        out_specs=[row_spec, pl.BlockSpec(part_shape, lambda h: (0,) * 6)],
        out_shape=[row_shape, jax.ShapeDtypeStruct(part_shape, F32)],
        scratch_shapes=[pltpu.VMEM((rows, head_dim), BF16), pltpu.VMEM((rows, head_dim), BF16),
                        pltpu.VMEM((head_dim, rows), F32)],
        compiler_params=params,
        cost_estimate=pl.CostEstimate(flops=pairs * 10 * head_dim, bytes_accessed=3 * kv_bytes, transcendentals=pairs),
        name="attention_backward",
    )
    return forward, backward


def weight_grads_kernel(count, heads, head_dim, x_ref, *refs):
    for g_ref, out_ref in zip(refs[:count], refs[count:]):
        grad = dot(x_ref[...], g_ref[...], TN)
        for h in range(heads):
            out_ref[:, h, :] = grad[:, h * head_dim:(h + 1) * head_dim]


def weight_grads(x, gs, heads):
    tok, width = x.shape
    head_dim = gs[0].shape[1] // heads
    block = min(512, width)
    return pl.pallas_call(
        functools.partial(weight_grads_kernel, len(gs), heads, head_dim),
        grid=(width // block,),
        in_specs=[pl.BlockSpec((tok, block), lambda i: (0, i))] + [pl.BlockSpec(g.shape, lambda i: (0, 0)) for g in gs],
        out_specs=[pl.BlockSpec((block, heads, head_dim), lambda i: (i, 0, 0)) for _ in gs],
        out_shape=[jax.ShapeDtypeStruct((width, heads, head_dim), F32) for _ in gs],
        compiler_params=pltpu.CompilerParams(dimension_semantics=("arbitrary",)),
        cost_estimate=pl.CostEstimate(flops=2 * tok * width * heads * head_dim * len(gs),
                                      bytes_accessed=4 * width * heads * head_dim * len(gs), transcendentals=0),
        name="weight_grads",
    )(x, *gs)


def solution(mesh):
    devs = mesh.shape["cp"]
    row_spec = P(("dp", "cp"), None)
    rep_spec = P(None, None, None)
    part_spec = P("dp", None, None)
    plane = devs // PLANES
    plane_groups = [[z * plane + i for i in range(plane)] for z in range(PLANES)]

    def to_plane(value, step):
        return lax.ppermute(value, "cp", [(i, (i // plane ^ step) * plane + i % plane) for i in range(devs)])

    def device_layer(hidden, grad_out, w_query, w_key, w_value, w_out):
        tok, width = hidden.shape
        heads, head_dim = w_query.shape[1:]
        kv_heads = w_key.shape[1]
        group = heads // kv_heads
        wide = group * head_dim
        forward, backward = attention_calls(devs, tok, group, head_dim)
        wq = w_query.reshape(width, heads * head_dim)
        wk = w_key.reshape(width, kv_heads * head_dim)
        wv = w_value.reshape(width, kv_heads * head_dim)
        wo = w_out.reshape(heads * head_dim, width)
        upper = lax.axis_index("cp") // plane >= PLANES // 2

        def mine_and_other(rows):
            first, second = jnp.split(rows, 2, axis=1)
            return jnp.where(upper, second, first), jnp.where(upper, first, second)

        def in_head_order(mine, other):
            return jnp.concatenate([jnp.where(upper, other, mine), jnp.where(upper, mine, other)], axis=1)

        key_mine, key_other = mine_and_other(dot(hidden, wk, NN).astype(BF16))
        value_mine, value_other = mine_and_other(dot(hidden, wv, NN).astype(BF16))
        kv_mine = jnp.concatenate([key_mine, value_mine], axis=1)
        kv_other = to_plane(jnp.concatenate([key_other, value_other], axis=1), PLANES - 1)
        near = jnp.concatenate([kv_mine, kv_other], axis=0)
        far = to_plane(near, 1)
        kv_local = jnp.concatenate([kv_mine, far, kv_other], axis=0)
        kv_local = with_layout_constraint(kv_local, Layout(major_to_minor=(0, 1)))
        kv_all = lax.all_gather(kv_local, "cp", axis=0, tiled=True, axis_index_groups=plane_groups)
        kv_all = with_layout_constraint(kv_all, Layout(major_to_minor=(0, 1)))
        kv_blocks = kv_all.reshape(plane, PLANES, 2, tok // 2, 2 * head_dim)

        query_mine, query_other = mine_and_other(dot(hidden, wq, NN).astype(BF16))
        dout_mine, dout_other = mine_and_other(dot(grad_out, wo, NT).astype(BF16))
        query = jnp.stack([query_mine, to_plane(query_other, PLANES - 1)])
        dout = jnp.stack([dout_mine, to_plane(dout_other, PLANES - 1)])
        att_parts, stats = forward(query, kv_blocks, dout)
        dq_parts, kv_part = backward(query, kv_blocks, dout, stats)

        slot_rows = 2 * tok
        kv_part = kv_part.reshape(plane * PLANES * slot_rows, head_dim)
        kv_part = lax.psum_scatter(kv_part, "cp", scatter_dimension=0, tiled=True, axis_index_groups=plane_groups)
        attended = in_head_order(att_parts[0], to_plane(att_parts[1], PLANES - 1))
        query_grad = in_head_order(dq_parts[0], to_plane(dq_parts[1], PLANES - 1))
        out_part = dot(attended, grad_out, TN).reshape(heads, head_dim, width)
        query_part, = weight_grads(hidden, [query_grad], heads)
        output = jnp.dot(attended, wo, preferred_element_type=F32).astype(BF16)
        hidden_part = dot(query_grad, wq, NT)
        kv_part, out_part, query_part, output, hidden_part = lax.optimization_barrier(
            (kv_part, out_part, query_part, output, hidden_part))

        slots = kv_part.reshape(PLANES, slot_rows, head_dim)
        mine = slots[0] + to_plane(slots[1], 1)
        other = to_plane(slots[2], 2) + to_plane(slots[3], 3)
        kv_grad = in_head_order(mine, other).astype(BF16)
        key_grad, value_grad = kv_grad[:tok], kv_grad[tok:]
        key_part, value_part = weight_grads(hidden, [key_grad, value_grad], kv_heads)
        grads = lax.psum((query_part, key_part, value_part, out_part), "cp")
        grad_hidden = (hidden_part + dot(key_grad, wk, NT) + dot(value_grad, wv, NT)).astype(BF16)
        return (output, grad_hidden, *grads)

    return jax.shard_map(
        device_layer,
        mesh=mesh,
        in_specs=(row_spec, row_spec, rep_spec, rep_spec, rep_spec, rep_spec),
        out_specs=(row_spec, row_spec, part_spec, part_spec, part_spec, part_spec),
        check_vma=False,
    )
```
